32 devices in a mesh: row: 16 (over z, y, core), col: 2 (over x).
Axes of the slice: x: 2, y: 2, z: 4, core: 2. Of those that a mesh axis runs over, the one named last changes fastest.
Arguments:
- vectors: float32 [1024, 32768], P(('row', 'col')), may hold values from -6 to 6
- reflectors: float32 [6, 128, 32768], P(None, 'col', 'row')
- factors: float32 [6, 128, 128], replicated, as said below
Outputs:
- transformed: float32 [1024, 32768], P('col', 'row')
The draws below stay inside these ranges and needn't reach their ends.
Inputs may be any that keep to these rules, and one draw needn't show every extreme that they name: factors[k] is upper triangular, and its inverse equals the strict upper part of reflectors[k] reflectors[k]^T plus half of that product's diagonal, so each panel is orthogonal.
All inputs are finite; a program needn't handle non-finite values.
Results may differ from the reference program's by a relative error of at most 0.0001.
Values sent between devices are 32-bit elements; how exact they have to be, the bound alone decides.
A program may use at most 128 MiB of HBM per device.

```python
import jax
import jax.numpy as jnp
from jax import lax

N = 32768
BLOCK = 128
PANELS = 6
EIGVECS = 1024


def invert_upper(matrix):
    identity = jnp.eye(matrix.shape[0], dtype=jnp.float32)
    return jax.scipy.linalg.solve_triangular(matrix, identity, lower=False)


def reflector_pair(key):
    random_part = jax.random.normal(jax.random.fold_in(key, 11), (PANELS, BLOCK, N), jnp.float32) / jnp.sqrt(jnp.float32(N))
    mixing = jnp.eye(BLOCK, dtype=jnp.float32) + 0.35 / jnp.sqrt(jnp.float32(BLOCK)) * jax.random.normal(jax.random.fold_in(key, 12), (PANELS, BLOCK, BLOCK), jnp.float32)
    reflect = jnp.einsum('pij,pjn->pin', mixing, random_part, precision=lax.Precision.HIGHEST)
    gram_matrix = jnp.einsum('pin,pjn->pij', reflect, reflect, precision=lax.Precision.HIGHEST)
    diagonal_half = 0.5 * jnp.einsum('pii->pi', gram_matrix)
    inverse = jnp.triu(gram_matrix, 1) + jax.vmap(jnp.diag)(diagonal_half)
    triangle = jax.vmap(invert_upper)(inverse)
    return (reflect, triangle)


def draw_reflectors(key, part):
    return reflector_pair(jax.random.fold_in(key, 7))[0]


def draw_factors(key, part):
    return reflector_pair(jax.random.fold_in(key, 7))[1]


def levels(own_key, extent, cuts, low, largest):
    gain = 1.0
    for position, shards_of in cuts:
        steps = jax.random.uniform(jax.random.fold_in(jax.random.fold_in(own_key, 6), position), (shards_of,), jnp.float32, low / len(cuts), largest / len(cuts))
        gain = gain * jnp.repeat(jnp.exp(steps), extent[position] // shards_of).reshape((-1,) + (1,) * (len(extent) - 1 - position))
    return gain


def gaussian(rng, extent, width, limit, pieces=(), kind=jnp.bfloat16):
    result = jax.random.normal(rng, extent, jnp.float32) * width
    if len(pieces) > 0:
        result = levels(rng, extent, pieces, -0.22, 0.18) * result
    return jnp.clip(result, min=-limit, max=limit).astype(kind)


def setup_inputs(seed: int = 0) -> dict:
    keys = jax.random.split(jax.random.key(seed), 4)
    return {
        "vectors": gaussian(keys[0], (EIGVECS, N), 1.0, 6.0, ((0, 32),), jnp.float32),
        "reflectors": draw_reflectors(jax.random.fold_in(keys[3], 71), 0),
        "factors": draw_factors(jax.random.fold_in(keys[3], 71), 0),
    }


def reference(vectors, reflectors, factors):
    current = vectors
    for panel in range(PANELS - 1, -1, -1):
        stacked = reflectors[panel]
        projection = lax.dot_general(current.astype(jnp.float32), stacked.astype(jnp.float32), (((1,), (1,)), ((), ())), precision=lax.Precision.HIGHEST, preferred_element_type=jnp.float32)
        update = jnp.dot(projection.astype(jnp.float32), factors[panel].T.astype(jnp.float32), precision=lax.Precision.HIGHEST, preferred_element_type=jnp.float32)
        current = current - jnp.dot(update.astype(jnp.float32), stacked.astype(jnp.float32), precision=lax.Precision.HIGHEST, preferred_element_type=jnp.float32)
    return current
```

```python
import functools

import jax
import jax.numpy as jnp
from jax import lax
from jax.experimental import pallas as pl
from jax.experimental.pallas import tpu as pltpu
from jax.sharding import PartitionSpec as P

MESH = pl.DeviceIdType.MESH
HIGH = lax.Precision.HIGH


def nt(left, right, precision):
    return lax.dot_general(
        left,
        right,
        (((1,), (1,)), ((), ())),
        precision=precision,
        preferred_element_type=jnp.float32,
    )


def split(value):
    top = value.astype(jnp.bfloat16)
    return top, (value - top.astype(jnp.float32)).astype(jnp.bfloat16)


def plain_nt(left, right):
    return lax.dot_general(
        left, right, (((1,), (1,)), ((), ())), preferred_element_type=jnp.float32
    )


def strides_of(rows):
    found = []
    stride = 1
    while stride < rows:
        found.append(stride)
        stride *= 2
    return found


def orders_of(rows):
    base = strides_of(rows)
    return [base, base[:1] + base[2:] + base[1:2]]


class Reduce:
    def __init__(self, row, row_count, source, landing, out, sems):
        self.row = row
        self.source = source
        self.landing = landing
        self.out = out
        self.sems = sems
        total = source.shape[0]
        self.orders = orders_of(row_count)
        self.part = total // len(self.orders)
        self.previous = [source.at[pl.ds(i * self.part, self.part)] for i in range(2)]
        self.offset = [i * self.part for i in range(2)]
        self.count = len(self.orders[0])
        self.pending = None

    def bit(self, stride):
        return lax.rem(self.row // stride, 2)

    def partner(self, stride):
        return self.row + stride * (1 - 2 * self.bit(stride))

    def copy(self, source, target, number, stride):
        return pltpu.make_async_remote_copy(
            src_ref=source,
            dst_ref=target,
            send_sem=self.sems.at[0, number],
            recv_sem=self.sems.at[1, number],
            device_id={"row": self.partner(stride)},
            device_id_type=MESH,
        )

    def halve_start(self, stage):
        self.pending = []
        half = self.part >> (stage + 1)
        start = self.part - (self.part >> stage)
        for i in range(2):
            stride = self.orders[i][stage]
            bit = self.bit(stride)
            away = pl.ds(pl.multiple_of((1 - bit) * half, 8), half)
            here = self.landing.at[i, pl.ds(start, half)]
            item = self.copy(self.previous[i].at[away], here, stage * 2 + i, stride)
            item.start()
            self.pending.append((item, here, bit, half))

    def halve_end(self):
        for i in range(2):
            item, here, bit, half = self.pending[i]
            item.wait()
            keep = pl.ds(pl.multiple_of(bit * half, 8), half)
            here[...] = here[...] + self.previous[i][keep, :]
            self.previous[i] = here
            self.offset[i] = self.offset[i] + bit * half

    def place(self, i, value):
        size = value.shape[0]
        self.out[pl.ds(pl.multiple_of(self.offset[i], 8), size), :] = value

    def double_start(self, stage):
        self.pending = []
        size = self.part >> (self.count - stage)
        for i in range(2):
            stride = self.orders[i][self.count - 1 - stage]
            where = self.out.at[pl.ds(pl.multiple_of(self.offset[i], 8), size)]
            item = self.copy(where, where, (self.count + stage) * 2 + i, stride)
            item.start()
            self.pending.append((item, self.bit(stride) * size))

    def double_end(self):
        for i in range(2):
            item, back = self.pending[i]
            item.wait()
            self.offset[i] = self.offset[i] - back


def exchange_kernel(
    row_count, col_count, vectors, reflectors, current, panels, gram,
    stage, held, tops, lows, partial, landing,
    row_sems, far_sems, gather_sems, local_sems, gram_sems,
):
    row = lax.axis_index("row")
    col = lax.axis_index("col")
    local = vectors.shape[0]
    length = current.shape[1]
    count, part, _ = reflectors.shape
    width = part * col_count

    barrier = pltpu.get_barrier_semaphore()
    for step in range(1, row_count):
        pl.semaphore_signal(
            barrier, inc=1, device_id={"row": lax.rem(row + step, row_count)}, device_id_type=MESH
        )
    for step in range(1, col_count):
        pl.semaphore_signal(
            barrier, inc=1, device_id={"col": lax.rem(col + step, col_count)}, device_id_type=MESH
        )
    pl.semaphore_wait(barrier, row_count + col_count - 2)

    def slot_rows(slot):
        return pl.ds(pl.multiple_of(slot * local, 8), local)

    gathers = []
    for step in range(1, col_count):
        for panel in range(count):
            number = (step - 1) * count + panel
            item = pltpu.make_async_remote_copy(
                src_ref=reflectors.at[panel],
                dst_ref=held.at[pl.ds(pl.multiple_of(panel * width + col * part, 8), part)],
                send_sem=gather_sems.at[0, number],
                recv_sem=gather_sems.at[1, number],
                device_id={"col": lax.rem(col + step, col_count)},
                device_id_type=MESH,
            )
            item.start()
            gathers.append(item)

    middle = row_count // 2
    steps = sorted(range(1, row_count), key=lambda step: (abs(step - middle), step))
    mine = row * col_count + col
    my_target = mine // row_count
    my_slot = lax.rem(mine, row_count)
    sends = {}
    for step in steps:
        other = lax.rem(row + step, row_count)
        source = vectors.at[:, pl.ds(pl.multiple_of(other * length, 128), length)]

        def sending(target, source=source, step=step, other=other):
            return pltpu.make_async_remote_copy(
                src_ref=source,
                dst_ref=target,
                send_sem=row_sems.at[0, step],
                recv_sem=row_sems.at[1, step],
                device_id={"row": other},
                device_id_type=MESH,
            )

        @pl.when(my_target == col)
        def _():
            sending(current.at[slot_rows(my_slot)]).start()

        @pl.when(my_target != col)
        def _():
            sending(stage.at[row]).start()

        sends[step] = sending(stage.at[row])

    own = pltpu.make_async_copy(
        vectors.at[:, pl.ds(pl.multiple_of(row * length, 128), length)], stage.at[row], local_sems.at[0]
    )
    own.start()
    own_panels = []
    for panel in range(count):
        item = pltpu.make_async_copy(
            reflectors.at[panel],
            held.at[pl.ds(pl.multiple_of(panel * width + col * part, 8), part)],
            local_sems.at[1 + panel],
        )
        item.start()
        own_panels.append(item)

    def onward(source_row):
        block = source_row * col_count + col
        target = block // row_count
        slot = lax.rem(block, row_count)
        return target, pltpu.make_async_remote_copy(
            src_ref=stage.at[source_row],
            dst_ref=current.at[slot_rows(slot)],
            send_sem=far_sems.at[0, slot],
            recv_sem=far_sems.at[1, slot],
            device_id={"col": target},
            device_id_type=MESH,
        )

    own.wait()
    own_target, own_far = onward(row)
    own_here = pltpu.make_async_copy(stage.at[row], current.at[slot_rows(my_slot)], local_sems.at[0])

    @pl.when(own_target == col)
    def _():
        own_here.start()
        own_here.wait()

    @pl.when(own_target != col)
    def _():
        own_far.start()

    def arrive(step):
        source_row = lax.rem(row - step + row_count, row_count)
        target, far = onward(source_row)
        sends[step].wait_recv()

        @pl.when(target != col)
        def _():
            far.start()

    early = (len(steps) + 1) // 2
    for step in steps[:early]:
        arrive(step)
    for item in own_panels:
        item.wait()
    for item in gathers:
        item.wait()
    keep_panels = pltpu.make_async_copy(held, panels, local_sems.at[0])
    keep_panels.start()

    def split_rows(i, carry):
        rows = pl.ds(pl.multiple_of(i * 32, 32), 32)
        top, low = split(held[rows, :])
        tops[rows, :] = top
        lows[rows, :] = low
        return carry

    lax.fori_loop(0, count * width // 32, split_rows, 0)
    base = 0
    for panel in range(count - 1):
        right = pl.ds(panel * width, width)

        def block(i, carry, right=right, base=base, panel=panel):
            left = pl.ds(pl.multiple_of((panel + 1 + i) * width, 128), width)
            value = plain_nt(tops[left, :], tops[right, :])
            value = value + plain_nt(tops[left, :], lows[right, :])
            value = value + plain_nt(lows[left, :], tops[right, :])
            partial[pl.ds(pl.multiple_of(base + i * width, 128), width), :] = value
            return carry

        lax.fori_loop(0, count - 1 - panel, block, 0)
        base += (count - 1 - panel) * width
    partial[pl.ds(base, partial.shape[0] - base), :] = jnp.zeros(
        (partial.shape[0] - base, width), jnp.float32
    )

    late = list(steps[early:])
    reduce = Reduce(row, row_count, partial, landing, gram, gram_sems)
    rounds = 2 * reduce.count
    done = 0
    for number in range(rounds):
        if number < reduce.count:
            reduce.halve_start(number)
        else:
            if number == reduce.count:
                for i in range(2):
                    reduce.place(i, reduce.previous[i][...])
            reduce.double_start(number - reduce.count)
        goal = len(late) * (number + 1) // rounds
        for step in late[done:goal]:
            arrive(step)
        done = goal
        if number < reduce.count:
            reduce.halve_end()
        else:
            reduce.double_end()

    keep_panels.wait()
    for step in steps:
        sends[step].wait_send()
    for source_row in range(row_count):
        target, far = onward(source_row)

        @pl.when(target != col)
        def _():
            far.wait_send()

    for slot in range(row_count):
        far = pltpu.make_async_remote_copy(
            src_ref=stage.at[0],
            dst_ref=current.at[slot_rows(slot)],
            send_sem=far_sems.at[0, slot],
            recv_sem=far_sems.at[1, slot],
            device_id={"col": col},
            device_id_type=MESH,
        )

        @pl.when(lax.rem(col * row_count + slot, col_count) != col)
        def _():
            far.wait_recv()


def solve_kernel(row_count, projection, gram, factors, update, landing, sems):
    row = lax.axis_index("row")
    barrier = pltpu.get_barrier_semaphore()
    for stride in strides_of(row_count):
        other = row + stride * (1 - 2 * lax.rem(row // stride, 2))
        pl.semaphore_signal(barrier, inc=1, device_id={"row": other}, device_id_type=MESH)
    pl.semaphore_wait(barrier, len(strides_of(row_count)))
    count, width, _ = factors.shape
    reduce = Reduce(row, row_count, projection, landing, update, sems)
    for stage in range(reduce.count):
        reduce.halve_start(stage)
        reduce.halve_end()
    value = jnp.concatenate([reduce.previous[i][...] for i in range(2)], axis=0)
    starts = []
    base = 0
    for panel in range(count):
        starts.append(base)
        base += (count - 1 - panel) * width
    solved = None
    for panel in range(count - 1, -1, -1):
        term = value[:, panel * width : (panel + 1) * width]
        if solved is not None:
            rows = (count - 1 - panel) * width
            term = term - jnp.dot(
                solved,
                gram[pl.ds(starts[panel], rows), :],
                precision=lax.Precision.HIGHEST,
                preferred_element_type=jnp.float32,
            )
        piece = nt(term, factors[panel], lax.Precision.HIGHEST)
        solved = piece if solved is None else jnp.concatenate([piece, solved], axis=1)
    size = value.shape[0] // 2
    for i in range(2):
        reduce.place(i, solved[i * size : (i + 1) * size, :])
    for stage in range(reduce.count):
        reduce.double_start(stage)
        reduce.double_end()


def on_device(vectors, reflectors, factors):
    local_count, total_length = vectors.shape
    row_count = lax.axis_size("row")
    col_count = lax.axis_size("col")
    length = total_length // row_count
    count, part, _ = reflectors.shape
    width = part * col_count
    rows = local_count * row_count
    stages = len(strides_of(row_count))
    unit = 16 * row_count
    gram_rows = -(-(count * (count - 1) // 2 * width) // unit) * unit
    anywhere = pl.BlockSpec(memory_space=pl.ANY)
    vmem = pl.BlockSpec(memory_space=pltpu.VMEM)
    dma = pltpu.SemaphoreType.DMA
    current, panels, gram = pl.pallas_call(
        functools.partial(exchange_kernel, row_count, col_count),
        name="exchange",
        out_shape=(
            jax.ShapeDtypeStruct((rows, length), jnp.float32),
            jax.ShapeDtypeStruct((count * width, length), jnp.float32),
            jax.ShapeDtypeStruct((gram_rows, width), jnp.float32),
        ),
        in_specs=[anywhere, anywhere],
        out_specs=(anywhere, anywhere, vmem),
        scratch_shapes=[
            pltpu.VMEM((row_count, local_count, length), jnp.float32),
            pltpu.VMEM((count * width, length), jnp.float32),
            pltpu.VMEM((count * width, length), jnp.bfloat16),
            pltpu.VMEM((count * width, length), jnp.bfloat16),
            pltpu.VMEM((gram_rows, width), jnp.float32),
            pltpu.VMEM((2, gram_rows // 2, width), jnp.float32),
            dma((2, row_count)),
            dma((2, row_count)),
            dma((2, (col_count - 1) * count)),
            dma((1 + count,)),
            dma((2, 4 * stages)),
        ],
        compiler_params=pltpu.CompilerParams(
            collective_id=0, has_side_effects=True, vmem_limit_bytes=48 * 1024 * 1024
        ),
    )(vectors, reflectors)
    projection = nt(current, panels, HIGH)
    update = pl.pallas_call(
        functools.partial(solve_kernel, row_count),
        name="solve",
        out_shape=jax.ShapeDtypeStruct((rows, count * width), jnp.float32),
        in_specs=[vmem, vmem, vmem],
        out_specs=vmem,
        scratch_shapes=[
            pltpu.VMEM((2, rows // 2, count * width), jnp.float32),
            dma((2, 4 * stages)),
        ],
        compiler_params=pltpu.CompilerParams(
            collective_id=1, has_side_effects=True, vmem_limit_bytes=32 * 1024 * 1024
        ),
    )(projection, gram, factors)
    return current - jnp.dot(update, panels, precision=HIGH, preferred_element_type=jnp.float32)


def solution(mesh):
    return jax.shard_map(
        on_device,
        mesh=mesh,
        in_specs=(P(("row", "col"), None), P(None, "col", "row"), P()),
        out_specs=P("col", "row"),
        check_vma=False,
    )
```

```python
import functools

import jax
import jax.numpy as jnp
from jax import lax
from jax.experimental import pallas as pl
from jax.experimental.pallas import tpu as pltpu
from jax.sharding import PartitionSpec as P

MESH = pl.DeviceIdType.MESH
HIGH = lax.Precision.HIGH


def nt(left, right, precision):
    return lax.dot_general(
        left,
        right,
        (((1,), (1,)), ((), ())),
        precision=precision,
        preferred_element_type=jnp.float32,
    )


def split(value):
    top = value.astype(jnp.bfloat16)
    return top, (value - top.astype(jnp.float32)).astype(jnp.bfloat16)


def plain_nt(left, right):
    return lax.dot_general(
        left, right, (((1,), (1,)), ((), ())), preferred_element_type=jnp.float32
    )


def strides_of(rows):
    found = []
    stride = 1
    while stride < rows:
        found.append(stride)
        stride *= 2
    return found


def orders_of(rows):
    base = strides_of(rows)
    return [base, base[:1] + base[2:] + base[1:2]]


class Reduce:
    def __init__(self, row, row_count, source, landing, out, sems):
        self.row = row
        self.source = source
        self.landing = landing
        self.out = out
        self.sems = sems
        total = source.shape[0]
        self.orders = orders_of(row_count)
        self.part = total // len(self.orders)
        self.previous = [source.at[pl.ds(i * self.part, self.part)] for i in range(2)]
        self.offset = [i * self.part for i in range(2)]
        self.count = len(self.orders[0])
        self.pending = None

    def bit(self, stride):
        return lax.rem(self.row // stride, 2)

    def partner(self, stride):
        return self.row + stride * (1 - 2 * self.bit(stride))

    def copy(self, source, target, number, stride):
        return pltpu.make_async_remote_copy(
            src_ref=source,
            dst_ref=target,
            send_sem=self.sems.at[0, number],
            recv_sem=self.sems.at[1, number],
            device_id={"row": self.partner(stride)},
            device_id_type=MESH,
        )

    def halve_start(self, stage):
        self.pending = []
        half = self.part >> (stage + 1)
        start = self.part - (self.part >> stage)
        for i in range(2):
            stride = self.orders[i][stage]
            bit = self.bit(stride)
            away = pl.ds(pl.multiple_of((1 - bit) * half, 8), half)
            here = self.landing.at[i, pl.ds(start, half)]
            item = self.copy(self.previous[i].at[away], here, stage * 2 + i, stride)
            item.start()
            self.pending.append((item, here, bit, half))

    def halve_end(self):
        for i in range(2):
            item, here, bit, half = self.pending[i]
            item.wait()
            keep = pl.ds(pl.multiple_of(bit * half, 8), half)
            here[...] = here[...] + self.previous[i][keep, :]
            self.previous[i] = here
            self.offset[i] = self.offset[i] + bit * half

    def place(self, i, value):
        size = value.shape[0]
        self.out[pl.ds(pl.multiple_of(self.offset[i], 8), size), :] = value

    def double_start(self, stage):
        self.pending = []
        size = self.part >> (self.count - stage)
        for i in range(2):
            stride = self.orders[i][self.count - 1 - stage]
            where = self.out.at[pl.ds(pl.multiple_of(self.offset[i], 8), size)]
            item = self.copy(where, where, (self.count + stage) * 2 + i, stride)
            item.start()
            self.pending.append((item, self.bit(stride) * size))

    def double_end(self):
        for i in range(2):
            item, back = self.pending[i]
            item.wait()
            self.offset[i] = self.offset[i] - back


def kernel(
    row_count, col_count, vectors, reflectors, factors, current, panels, update,
    stage, held, tops, lows, here, here_top, here_low, projection, solved_rows,
    landing, partial, gram, gram_landing,
    row_sems, far_sems, gather_sems, local_sems, out_sems, gram_sems, first_sems, second_sems,
):
    row = lax.axis_index("row")
    col = lax.axis_index("col")
    local = vectors.shape[0]
    length = current.shape[1]
    count, part, _ = reflectors.shape
    width = part * col_count
    group = row_count // col_count
    half_slots = row_count // 2
    half_rows = half_slots * local

    barrier = pltpu.get_barrier_semaphore()
    for step in range(1, row_count):
        pl.semaphore_signal(
            barrier, inc=1, device_id={"row": lax.rem(row + step, row_count)}, device_id_type=MESH
        )
    for step in range(1, col_count):
        pl.semaphore_signal(
            barrier, inc=1, device_id={"col": lax.rem(col + step, col_count)}, device_id_type=MESH
        )
    pl.semaphore_wait(barrier, row_count + col_count - 2)

    def slot_rows(slot):
        return pl.ds(pl.multiple_of(slot * local, 8), local)

    gathers = []
    for step in range(1, col_count):
        for panel in range(count):
            number = (step - 1) * count + panel
            item = pltpu.make_async_remote_copy(
                src_ref=reflectors.at[panel],
                dst_ref=held.at[pl.ds(pl.multiple_of(panel * width + col * part, 8), part)],
                send_sem=gather_sems.at[0, number],
                recv_sem=gather_sems.at[1, number],
                device_id={"col": lax.rem(col + step, col_count)},
                device_id_type=MESH,
            )
            item.start()
            gathers.append(item)

    def onward(source_row):
        block = source_row * col_count + col
        target = block // row_count
        slot = lax.rem(block, row_count)
        place = lax.rem(slot - target + col_count, col_count) * group + slot // col_count
        return target, place

    middle = row_count // 2
    steps = sorted(range(1, row_count), key=lambda step: (abs(step - middle), step))
    my_target, my_place = onward(row)
    sends = {}
    for step in steps:
        other = lax.rem(row + step, row_count)
        source = vectors.at[:, pl.ds(pl.multiple_of(other * length, 128), length)]

        def sending(target, source=source, step=step, other=other):
            return pltpu.make_async_remote_copy(
                src_ref=source,
                dst_ref=target,
                send_sem=row_sems.at[0, step],
                recv_sem=row_sems.at[1, step],
                device_id={"row": other},
                device_id_type=MESH,
            )

        @pl.when(my_target == col)
        def _():
            sending(here.at[slot_rows(my_place)]).start()

        @pl.when(my_target != col)
        def _():
            sending(stage.at[row]).start()

        sends[step] = sending(stage.at[row])

    own = pltpu.make_async_copy(
        vectors.at[:, pl.ds(pl.multiple_of(row * length, 128), length)], stage.at[row], local_sems.at[0]
    )
    own.start()
    own_panels = []
    for panel in range(count):
        item = pltpu.make_async_copy(
            reflectors.at[panel],
            held.at[pl.ds(pl.multiple_of(panel * width + col * part, 8), part)],
            local_sems.at[1 + panel],
        )
        item.start()
        own_panels.append(item)

    def far_copy(source_row):
        target, place = onward(source_row)
        return target, pltpu.make_async_remote_copy(
            src_ref=stage.at[source_row],
            dst_ref=here.at[slot_rows(place)],
            send_sem=far_sems.at[0, place],
            recv_sem=far_sems.at[1, place],
            device_id={"col": target},
            device_id_type=MESH,
        )

    own.wait()
    own_target, own_far = far_copy(row)
    own_here = pltpu.make_async_copy(stage.at[row], here.at[slot_rows(my_place)], local_sems.at[0])

    @pl.when(own_target == col)
    def _():
        own_here.start()
        own_here.wait()

    @pl.when(own_target != col)
    def _():
        own_far.start()

    def arrive(step):
        target, far = far_copy(lax.rem(row - step + row_count, row_count))
        sends[step].wait_recv()

        @pl.when(target != col)
        def _():
            far.start()

    early = (len(steps) + 1) // 2
    for step in steps[:early]:
        arrive(step)
    for item in own_panels:
        item.wait()
    for item in gathers:
        item.wait()
    keep_panels = pltpu.make_async_copy(held, panels, local_sems.at[0])
    keep_panels.start()

    def split_rows(i, carry):
        rows = pl.ds(pl.multiple_of(i * 32, 32), 32)
        top, low = split(held[rows, :])
        tops[rows, :] = top
        lows[rows, :] = low
        return carry

    lax.fori_loop(0, count * width // 32, split_rows, 0)
    base = 0
    starts = []
    for panel in range(count):
        starts.append(base)
        right = pl.ds(panel * width, width)

        def block(i, carry, right=right, base=base, panel=panel):
            left = pl.ds(pl.multiple_of((panel + 1 + i) * width, 128), width)
            value = plain_nt(tops[left, :], tops[right, :])
            value = value + plain_nt(tops[left, :], lows[right, :])
            value = value + plain_nt(lows[left, :], tops[right, :])
            partial[pl.ds(pl.multiple_of(base + i * width, 128), width), :] = value
            return carry

        if panel < count - 1:
            lax.fori_loop(0, count - 1 - panel, block, 0)
        base += (count - 1 - panel) * width
    partial[pl.ds(base, partial.shape[0] - base), :] = jnp.zeros(
        (partial.shape[0] - base, width), jnp.float32
    )

    def put_out(source, target, place, which):
        slot = (place % group) * col_count + lax.rem(col + place // group, col_count)
        item = pltpu.make_async_copy(
            source.at[slot_rows(place)], target.at[slot_rows(slot)], out_sems.at[which, place]
        )
        item.start()
        return item

    outs = []
    tile = 2 * width if count % 2 == 0 else width

    def project(chunk):
        for place in range(chunk * half_slots, (chunk + 1) * half_slots):
            if place >= group:
                pltpu.make_async_remote_copy(
                    src_ref=stage.at[0],
                    dst_ref=here.at[slot_rows(place)],
                    send_sem=far_sems.at[0, place],
                    recv_sem=far_sems.at[1, place],
                    device_id={"col": col},
                    device_id_type=MESH,
                ).wait_recv()
            outs.append(put_out(here, current, place, 0))

        def split_here(i, carry):
            rows = pl.ds(pl.multiple_of(i * 32, 32), 32)
            top, low = split(here[pl.ds(pl.multiple_of(chunk * half_rows + i * 32, 32), 32), :])
            here_top[rows, :] = top
            here_low[rows, :] = low
            return carry

        lax.fori_loop(0, half_rows // 32, split_here, 0)

        def columns(i, carry):
            right = pl.ds(pl.multiple_of(i * tile, 128), tile)
            value = plain_nt(here_top[...], tops[right, :])
            value = value + plain_nt(here_top[...], lows[right, :])
            value = value + plain_nt(here_low[...], tops[right, :])
            projection[pl.ds(chunk * half_rows, half_rows), right] = value
            return carry

        lax.fori_loop(0, count * width // tile, columns, 0)

    def solve(reduce):
        value = jnp.concatenate([reduce.previous[i][...] for i in range(2)], axis=0)
        solved = None
        for panel in range(count - 1, -1, -1):
            term = value[:, panel * width : (panel + 1) * width]
            if solved is not None:
                rows = (count - 1 - panel) * width
                term = term - jnp.dot(
                    solved,
                    gram[pl.ds(starts[panel], rows), :],
                    precision=lax.Precision.HIGHEST,
                    preferred_element_type=jnp.float32,
                )
            piece = nt(term, factors[panel], lax.Precision.HIGHEST)
            solved = piece if solved is None else jnp.concatenate([piece, solved], axis=1)
        size = value.shape[0] // 2
        for i in range(2):
            reduce.place(i, solved[i * size : (i + 1) * size, :])

    def chunk_reduce(chunk, sems):
        rows = pl.ds(chunk * half_rows, half_rows)
        return Reduce(
            row, row_count, projection.at[rows], landing.at[chunk], solved_rows.at[rows], sems
        )

    late = list(steps[early:])
    inner = Reduce(row, row_count, partial, gram_landing, gram, gram_sems)
    stages = inner.count
    done = 0
    for number in range(stages):
        inner.halve_start(number)
        goal = len(late) * (number + 1) // stages
        for step in late[done:goal]:
            arrive(step)
        done = goal
        inner.halve_end()
    for i in range(2):
        inner.place(i, inner.previous[i][...])
    inner.double_start(0)
    project(0)
    inner.double_end()
    first = chunk_reduce(0, first_sems)
    for number in range(stages):
        first.halve_start(number)
        if number + 1 < stages:
            inner.double_start(number + 1)
            inner.double_end()
        first.halve_end()
    solve(first)
    first.double_start(0)
    project(1)
    first.double_end()
    second = chunk_reduce(1, second_sems)
    for number in range(stages):
        second.halve_start(number)
        if number + 1 < stages:
            first.double_start(number + 1)
            first.double_end()
        second.halve_end()
    for place in range(half_slots):
        outs.append(put_out(solved_rows, update, place, 1))
    solve(second)
    for number in range(stages):
        second.double_start(number)
        second.double_end()
    for place in range(half_slots, row_count):
        outs.append(put_out(solved_rows, update, place, 1))

    keep_panels.wait()
    for step in steps:
        sends[step].wait_send()
    for source_row in range(row_count):
        target, far = far_copy(source_row)

        @pl.when(target != col)
        def _():
            far.wait_send()

    for item in outs:
        item.wait()


def on_device(vectors, reflectors, factors):
    local_count, total_length = vectors.shape
    row_count = lax.axis_size("row")
    col_count = lax.axis_size("col")
    length = total_length // row_count
    count, part, _ = reflectors.shape
    width = part * col_count
    rows = local_count * row_count
    stages = len(strides_of(row_count))
    unit = 16 * row_count
    gram_rows = -(-(count * (count - 1) // 2 * width) // unit) * unit
    anywhere = pl.BlockSpec(memory_space=pl.ANY)
    vmem = pl.BlockSpec(memory_space=pltpu.VMEM)
    dma = pltpu.SemaphoreType.DMA
    single, half = jnp.float32, jnp.bfloat16
    current, panels, update = pl.pallas_call(
        functools.partial(kernel, row_count, col_count),
        name="exchange",
        out_shape=(
            jax.ShapeDtypeStruct((rows, length), single),
            jax.ShapeDtypeStruct((count * width, length), single),
            jax.ShapeDtypeStruct((rows, count * width), single),
        ),
        in_specs=[anywhere, anywhere, vmem],
        out_specs=(anywhere, anywhere, anywhere),
        scratch_shapes=[
            pltpu.VMEM((row_count, local_count, length), single),
            pltpu.VMEM((count * width, length), single),
            pltpu.VMEM((count * width, length), half),
            pltpu.VMEM((count * width, length), half),
            pltpu.VMEM((rows, length), single),
            pltpu.VMEM((rows // 2, length), half),
            pltpu.VMEM((rows // 2, length), half),
            pltpu.VMEM((rows, count * width), single),
            pltpu.VMEM((rows, count * width), single),
            pltpu.VMEM((2, 2, rows // 4, count * width), single),
            pltpu.VMEM((gram_rows, width), single),
            pltpu.VMEM((gram_rows, width), single),
            pltpu.VMEM((2, gram_rows // 2, width), single),
            dma((2, row_count)),
            dma((2, row_count)),
            dma((2, (col_count - 1) * count)),
            dma((1 + count,)),
            dma((2, row_count)),
            dma((2, 4 * stages)),
            dma((2, 4 * stages)),
            dma((2, 4 * stages)),
        ],
        compiler_params=pltpu.CompilerParams(
            collective_id=0, has_side_effects=True, vmem_limit_bytes=56 * 1024 * 1024
        ),
    )(vectors, reflectors, factors)
    return current - jnp.dot(update, panels, precision=HIGH, preferred_element_type=single)


def solution(mesh):
    return jax.shard_map(
        on_device,
        mesh=mesh,
        in_specs=(P(("row", "col"), None), P(None, "col", "row"), P()),
        out_specs=P("col", "row"),
        check_vma=False,
    )
```

```python
import functools

import jax
import jax.numpy as jnp
from jax import lax
from jax.experimental import pallas as pl
from jax.experimental.pallas import tpu as pltpu
from jax.sharding import PartitionSpec as P

MESH = pl.DeviceIdType.MESH
HIGH = lax.Precision.HIGH


def nt(left, right, precision):
    return lax.dot_general(
        left,
        right,
        (((1,), (1,)), ((), ())),
        precision=precision,
        preferred_element_type=jnp.float32,
    )


def split(value):
    top = value.astype(jnp.bfloat16)
    return top, (value - top.astype(jnp.float32)).astype(jnp.bfloat16)


def plain_nt(left, right):
    return lax.dot_general(
        left, right, (((1,), (1,)), ((), ())), preferred_element_type=jnp.float32
    )


def strides_of(rows):
    found = []
    stride = 1
    while stride < rows:
        found.append(stride)
        stride *= 2
    return found


def orders_of(rows):
    base = strides_of(rows)
    return [base, base[:1] + base[2:] + base[1:2]]


class Reduce:
    def __init__(self, row, row_count, source, landing, out, sems):
        self.row = row
        self.source = source
        self.landing = landing
        self.out = out
        self.sems = sems
        total = source.shape[0]
        self.orders = orders_of(row_count)
        self.part = total // len(self.orders)
        self.previous = [source.at[pl.ds(i * self.part, self.part)] for i in range(2)]
        self.offset = [i * self.part for i in range(2)]
        self.count = len(self.orders[0])
        self.pending = None

    def bit(self, stride):
        return lax.rem(self.row // stride, 2)

    def partner(self, stride):
        return self.row + stride * (1 - 2 * self.bit(stride))

    def copy(self, source, target, number, stride):
        return pltpu.make_async_remote_copy(
            src_ref=source,
            dst_ref=target,
            send_sem=self.sems.at[0, number],
            recv_sem=self.sems.at[1, number],
            device_id={"row": self.partner(stride)},
            device_id_type=MESH,
        )

    def halve_start(self, stage):
        self.pending = []
        half = self.part >> (stage + 1)
        start = self.part - (self.part >> stage)
        for i in range(2):
            stride = self.orders[i][stage]
            bit = self.bit(stride)
            away = pl.ds(pl.multiple_of((1 - bit) * half, 8), half)
            here = self.landing.at[i, pl.ds(start, half)]
            item = self.copy(self.previous[i].at[away], here, stage * 2 + i, stride)
            item.start()
            self.pending.append((item, here, bit, half))

    def halve_end(self):
        for i in range(2):
            item, here, bit, half = self.pending[i]
            item.wait()
            keep = pl.ds(pl.multiple_of(bit * half, 8), half)
            here[...] = here[...] + self.previous[i][keep, :]
            self.previous[i] = here
            self.offset[i] = self.offset[i] + bit * half

    def place(self, i, value):
        size = value.shape[0]
        self.out[pl.ds(pl.multiple_of(self.offset[i], 8), size), :] = value

    def double_start(self, stage):
        self.pending = []
        size = self.part >> (self.count - stage)
        for i in range(2):
            stride = self.orders[i][self.count - 1 - stage]
            where = self.out.at[pl.ds(pl.multiple_of(self.offset[i], 8), size)]
            item = self.copy(where, where, (self.count + stage) * 2 + i, stride)
            item.start()
            self.pending.append((item, self.bit(stride) * size))

    def double_end(self):
        for i in range(2):
            item, back = self.pending[i]
            item.wait()
            self.offset[i] = self.offset[i] - back


def kernel(
    row_count, col_count, vectors, reflectors, factors, current, panels, update,
    stage, held, tops, lows, here, here_top, here_low, projection, solved_rows,
    landing, partial, gram, gram_landing,
    row_sems, far_sems, gather_sems, local_sems, out_sems, gram_sems, first_sems, second_sems,
):
    row = lax.axis_index("row")
    col = lax.axis_index("col")
    local = vectors.shape[0]
    length = current.shape[1]
    count, part, _ = reflectors.shape
    width = part * col_count
    group = row_count // col_count
    half_slots = row_count // 2
    half_rows = half_slots * local

    barrier = pltpu.get_barrier_semaphore()
    for step in range(1, row_count):
        pl.semaphore_signal(
            barrier, inc=1, device_id={"row": lax.rem(row + step, row_count)}, device_id_type=MESH
        )
    for step in range(1, col_count):
        pl.semaphore_signal(
            barrier, inc=1, device_id={"col": lax.rem(col + step, col_count)}, device_id_type=MESH
        )
    pl.semaphore_wait(barrier, row_count + col_count - 2)

    def slot_rows(slot):
        return pl.ds(pl.multiple_of(slot * local, 8), local)

    gathers = []
    for step in range(1, col_count):
        for panel in range(count):
            number = (step - 1) * count + panel
            item = pltpu.make_async_remote_copy(
                src_ref=reflectors.at[panel],
                dst_ref=held.at[pl.ds(pl.multiple_of(panel * width + col * part, 8), part)],
                send_sem=gather_sems.at[0, number],
                recv_sem=gather_sems.at[1, number],
                device_id={"col": lax.rem(col + step, col_count)},
                device_id_type=MESH,
            )
            item.start()
            gathers.append(item)

    def onward(source_row):
        block = source_row * col_count + col
        target = block // row_count
        slot = lax.rem(block, row_count)
        place = lax.rem(slot - target + col_count, col_count) * group + slot // col_count
        return target, place

    middle = row_count // 2
    ranked = sorted(range(1, row_count), key=lambda step: (abs(step - middle), step))
    steps = []
    while ranked:
        steps.append(ranked.pop(0))
        if ranked:
            steps.append(ranked.pop())
    my_target, my_place = onward(row)
    sends = {}
    for step in steps:
        other = lax.rem(row + step, row_count)
        source = vectors.at[:, pl.ds(pl.multiple_of(other * length, 128), length)]

        def sending(target, source=source, step=step, other=other):
            return pltpu.make_async_remote_copy(
                src_ref=source,
                dst_ref=target,
                send_sem=row_sems.at[0, step],
                recv_sem=row_sems.at[1, step],
                device_id={"row": other},
                device_id_type=MESH,
            )

        @pl.when(my_target == col)
        def _():
            sending(here.at[slot_rows(my_place)]).start()

        @pl.when(my_target != col)
        def _():
            sending(stage.at[row]).start()

        sends[step] = sending(stage.at[row])

    own = pltpu.make_async_copy(
        vectors.at[:, pl.ds(pl.multiple_of(row * length, 128), length)], stage.at[row], local_sems.at[0]
    )
    own.start()
    own_panels = []
    for panel in range(count):
        item = pltpu.make_async_copy(
            reflectors.at[panel],
            held.at[pl.ds(pl.multiple_of(panel * width + col * part, 8), part)],
            local_sems.at[1 + panel],
        )
        item.start()
        own_panels.append(item)

    def far_copy(source_row):
        target, place = onward(source_row)
        return target, pltpu.make_async_remote_copy(
            src_ref=stage.at[source_row],
            dst_ref=here.at[slot_rows(place)],
            send_sem=far_sems.at[0, place],
            recv_sem=far_sems.at[1, place],
            device_id={"col": target},
            device_id_type=MESH,
        )

    own.wait()
    own_target, own_far = far_copy(row)
    own_here = pltpu.make_async_copy(stage.at[row], here.at[slot_rows(my_place)], local_sems.at[0])

    @pl.when(own_target == col)
    def _():
        own_here.start()
        own_here.wait()

    @pl.when(own_target != col)
    def _():
        own_far.start()

    def arrive(step):
        target, far = far_copy(lax.rem(row - step + row_count, row_count))
        sends[step].wait_recv()

        @pl.when(target != col)
        def _():
            far.start()

    early = len(steps) // 5
    for step in steps[:early]:
        arrive(step)
    for item in own_panels:
        item.wait()
    for item in gathers:
        item.wait()
    keep_panels = pltpu.make_async_copy(held, panels, local_sems.at[0])
    keep_panels.start()

    def split_rows(i, carry):
        rows = pl.ds(pl.multiple_of(i * 32, 32), 32)
        top, low = split(held[rows, :])
        tops[rows, :] = top
        lows[rows, :] = low
        return carry

    lax.fori_loop(0, count * width // 32, split_rows, 0)
    base = 0
    starts = []
    for panel in range(count):
        starts.append(base)
        right = pl.ds(panel * width, width)

        def block(i, carry, right=right, base=base, panel=panel):
            left = pl.ds(pl.multiple_of((panel + 1 + i) * width, 128), width)
            value = plain_nt(tops[left, :], tops[right, :])
            value = value + plain_nt(tops[left, :], lows[right, :])
            value = value + plain_nt(lows[left, :], tops[right, :])
            partial[pl.ds(pl.multiple_of(base + i * width, 128), width), :] = value
            return carry

        if panel < count - 1:
            lax.fori_loop(0, count - 1 - panel, block, 0)
        base += (count - 1 - panel) * width
    partial[pl.ds(base, partial.shape[0] - base), :] = jnp.zeros(
        (partial.shape[0] - base, width), jnp.float32
    )

    def put_out(source, target, place, which):
        slot = (place % group) * col_count + lax.rem(col + place // group, col_count)
        item = pltpu.make_async_copy(
            source.at[slot_rows(place)], target.at[slot_rows(slot)], out_sems.at[which, place]
        )
        item.start()
        return item

    outs = []
    tile = 2 * width if count % 2 == 0 else width

    def project(chunk):
        for place in range(chunk * half_slots, (chunk + 1) * half_slots):
            if place >= group:
                pltpu.make_async_remote_copy(
                    src_ref=stage.at[0],
                    dst_ref=here.at[slot_rows(place)],
                    send_sem=far_sems.at[0, place],
                    recv_sem=far_sems.at[1, place],
                    device_id={"col": col},
                    device_id_type=MESH,
                ).wait_recv()
            outs.append(put_out(here, current, place, 0))

        def split_here(i, carry):
            rows = pl.ds(pl.multiple_of(i * 32, 32), 32)
            top, low = split(here[pl.ds(pl.multiple_of(chunk * half_rows + i * 32, 32), 32), :])
            here_top[rows, :] = top
            here_low[rows, :] = low
            return carry

        lax.fori_loop(0, half_rows // 32, split_here, 0)

        def columns(i, carry):
            right = pl.ds(pl.multiple_of(i * tile, 128), tile)
            value = plain_nt(here_top[...], tops[right, :])
            value = value + plain_nt(here_top[...], lows[right, :])
            value = value + plain_nt(here_low[...], tops[right, :])
            projection[pl.ds(chunk * half_rows, half_rows), right] = value
            return carry

        lax.fori_loop(0, count * width // tile, columns, 0)

    def solve(reduce):
        value = jnp.concatenate([reduce.previous[i][...] for i in range(2)], axis=0)
        solved = None
        for panel in range(count - 1, -1, -1):
            term = value[:, panel * width : (panel + 1) * width]
            if solved is not None:
                rows = (count - 1 - panel) * width
                term = term - jnp.dot(
                    solved,
                    gram[pl.ds(starts[panel], rows), :],
                    precision=lax.Precision.HIGHEST,
                    preferred_element_type=jnp.float32,
                )
            piece = nt(term, factors[panel], lax.Precision.HIGHEST)
            solved = piece if solved is None else jnp.concatenate([piece, solved], axis=1)
        size = value.shape[0] // 2
        for i in range(2):
            reduce.place(i, solved[i * size : (i + 1) * size, :])

    def chunk_reduce(chunk, sems):
        rows = pl.ds(chunk * half_rows, half_rows)
        return Reduce(
            row, row_count, projection.at[rows], landing.at[chunk], solved_rows.at[rows], sems
        )

    late = list(steps[early:])
    inner = Reduce(row, row_count, partial, gram_landing, gram, gram_sems)
    stages = inner.count
    done = 0
    for number in range(stages):
        inner.halve_start(number)
        goal = len(late) * (number + 1) // stages
        for step in late[done:goal]:
            arrive(step)
        done = goal
        inner.halve_end()
    for i in range(2):
        inner.place(i, inner.previous[i][...])
    inner.double_start(0)
    project(0)
    inner.double_end()
    first = chunk_reduce(0, first_sems)
    for number in range(stages):
        first.halve_start(number)
        if number + 1 < stages:
            inner.double_start(number + 1)
            inner.double_end()
        first.halve_end()
    solve(first)
    first.double_start(0)
    project(1)
    first.double_end()
    second = chunk_reduce(1, second_sems)
    for number in range(stages):
        second.halve_start(number)
        if number + 1 < stages:
            first.double_start(number + 1)
            first.double_end()
        second.halve_end()
    for place in range(half_slots):
        outs.append(put_out(solved_rows, update, place, 1))
    solve(second)
    for number in range(stages):
        second.double_start(number)
        second.double_end()
    for place in range(half_slots, row_count):
        outs.append(put_out(solved_rows, update, place, 1))

    keep_panels.wait()
    for step in steps:
        sends[step].wait_send()
    for source_row in range(row_count):
        target, far = far_copy(source_row)

        @pl.when(target != col)
        def _():
            far.wait_send()

    for item in outs:
        item.wait()


def on_device(vectors, reflectors, factors):
    local_count, total_length = vectors.shape
    row_count = lax.axis_size("row")
    col_count = lax.axis_size("col")
    length = total_length // row_count
    count, part, _ = reflectors.shape
    width = part * col_count
    rows = local_count * row_count
    stages = len(strides_of(row_count))
    unit = 16 * row_count
    gram_rows = -(-(count * (count - 1) // 2 * width) // unit) * unit
    anywhere = pl.BlockSpec(memory_space=pl.ANY)
    vmem = pl.BlockSpec(memory_space=pltpu.VMEM)
    dma = pltpu.SemaphoreType.DMA
    single, half = jnp.float32, jnp.bfloat16
    current, panels, update = pl.pallas_call(
        functools.partial(kernel, row_count, col_count),
        name="exchange",
        out_shape=(
            jax.ShapeDtypeStruct((rows, length), single),
            jax.ShapeDtypeStruct((count * width, length), single),
            jax.ShapeDtypeStruct((rows, count * width), single),
        ),
        in_specs=[anywhere, anywhere, vmem],
        out_specs=(anywhere, anywhere, anywhere),
        scratch_shapes=[
            pltpu.VMEM((row_count, local_count, length), single),
            pltpu.VMEM((count * width, length), single),
            pltpu.VMEM((count * width, length), half),
            pltpu.VMEM((count * width, length), half),
            pltpu.VMEM((rows, length), single),
            pltpu.VMEM((rows // 2, length), half),
            pltpu.VMEM((rows // 2, length), half),
            pltpu.VMEM((rows, count * width), single),
            pltpu.VMEM((rows, count * width), single),
            pltpu.VMEM((2, 2, rows // 4, count * width), single),
            pltpu.VMEM((gram_rows, width), single),
            pltpu.VMEM((gram_rows, width), single),
            pltpu.VMEM((2, gram_rows // 2, width), single),
            dma((2, row_count)),
            dma((2, row_count)),
            dma((2, (col_count - 1) * count)),
            dma((1 + count,)),
            dma((2, row_count)),
            dma((2, 4 * stages)),
            dma((2, 4 * stages)),
            dma((2, 4 * stages)),
        ],
        compiler_params=pltpu.CompilerParams(
            collective_id=0, has_side_effects=True, vmem_limit_bytes=56 * 1024 * 1024
        ),
    )(vectors, reflectors, factors)
    return current - jnp.dot(update, panels, precision=HIGH, preferred_element_type=single)


def solution(mesh):
    return jax.shard_map(
        on_device,
        mesh=mesh,
        in_specs=(P(("row", "col"), None), P(None, "col", "row"), P()),
        out_specs=P("col", "row"),
        check_vma=False,
    )
```
